32 devices in a mesh: slab: 8 (over y, x, core), col: 4 (over z).
Axes of the slice: x: 2, y: 2, z: 4, core: 2. Of those that a mesh axis runs over, the one named last changes fastest.
Arguments:
- hamiltonian_blocks: bfloat16 [128, 9, 128, 128], P('slab'), may hold values from -0.0625 to 0.0625
- block_columns: int32 [128, 9], P('slab'), may hold values from 0 to 127, as said below
- probe: bfloat16 [16384, 2048], P('slab', 'col'), may hold values from -6 to 6
- previous: float32 [16384, 2048], P('slab', 'col'), may hold values from -6 to 6
- current: float32 [16384, 2048], P('slab', 'col'), may hold values from -6 to 6
- orbital_weight: float32 [16384], P('slab'), may hold values from 0.1 to 10
Outputs:
- last_previous: float32 [16384, 2048], P('slab', 'col')
- last_current: float32 [16384, 2048], P('slab', 'col')
- moments: float32 [3, 2048], P(None, 'col')
The draws below stay inside these ranges and needn't reach their ends.
Inputs may be any that keep to these rules, and one draw needn't show every extreme that they name: `block_columns`: the 9 entries of a row are distinct block columns within 5 of the row's own block row, counted cyclically modulo 128; they include the row itself and the block rows 5 before and 5 after it.
All inputs are finite; a program needn't handle non-finite values.
Results may differ from the reference program's by a relative error of at most 0.0024.
Values may be sent and summed in bfloat16 or wider, within the bound.
A program may use at most 192 MiB of HBM per device.

```python
import math
import jax
import jax.numpy as jnp
from jax import lax

BLK = 128
BAND = 5
NB = 9
TERMS = 3
NBR = 128
NORB = 16384
COLS = 2048


def draw_block_columns(key, part):
    count = 2 * BAND - 2
    scores = jax.random.randint(key, (NBR, count), 0, 1 << 20) * count + jnp.arange(count)[None, :]
    picked = jnp.argsort(scores, axis=1)[:, :NB - 3]
    offsets = jnp.where(picked < BAND - 1, picked - (BAND - 1), picked - BAND + 2)
    fixed_part = jnp.broadcast_to(jnp.array([0, -BAND, BAND], jnp.int32)[None, :], (NBR, 3))
    every = jnp.concatenate([fixed_part, offsets.astype(jnp.int32)], axis=1)
    rowid = jnp.arange(NBR, dtype=jnp.int32)[:, None]
    return ((rowid + every) % NBR).astype(jnp.int32)


def steps_of(own_key, extent, shards, low, largest):
    gain = 1.0
    for dim, shards_of in shards:
        draws = jax.random.uniform(jax.random.fold_in(jax.random.fold_in(own_key, 6), dim), (shards_of,), jnp.float32, low / len(shards), largest / len(shards))
        gain = gain * jnp.repeat(jnp.exp(draws), extent[dim] // shards_of).reshape((-1,) + (1,) * (len(extent) - 1 - dim))
    return gain


def centred(own_key, shape, deviation, most, pieces=(), kind=jnp.bfloat16):
    values = deviation * jax.random.normal(own_key, shape, jnp.float32)
    if pieces:
        values = values * steps_of(own_key, shape, pieces, -0.22, 0.18)
    return jnp.clip(values, -most, most).astype(kind)


def setup_inputs(seed: int = 0) -> dict:
    arg_keys = jax.random.split(jax.random.key(seed), 7)
    return {
        "hamiltonian_blocks": centred(arg_keys[0], (NBR, NB, BLK, BLK), (8 * NB * BLK) ** -0.5, 0.0625, ((0, 8),)),
        "block_columns": draw_block_columns(jax.random.fold_in(arg_keys[6], 71), 0),
        "probe": centred(arg_keys[2], (NORB, COLS), 1.0, 6.0, ((0, 8), (1, 4))),
        "previous": centred(arg_keys[3], (NORB, COLS), 1.0, 6.0, ((0, 8), (1, 4)), jnp.float32),
        "current": centred(arg_keys[4], (NORB, COLS), 1.0, 6.0, ((0, 8), (1, 4)), jnp.float32),
        "orbital_weight": jnp.clip(jnp.exp(math.log(10.0) - 4.6051702 * jax.random.uniform(arg_keys[5], (NORB,), jnp.float32) ** steps_of(arg_keys[5], (NORB,), ((0, 8),), -0.2, 0.2)), 0.1, 10.0),
    }


def reference(hamiltonian_blocks, block_columns, probe, previous, current, orbital_weight):
    total = hamiltonian_blocks.shape[0] * BLK
    weights = orbital_weight[:, None] * probe.astype(jnp.float32) / total
    results = []
    for term in range(TERMS):
        source = current.astype(jnp.bfloat16).reshape(NBR, BLK, -1)

        def one_row(pair):
            blocks, columns = pair
            picked = source[columns]
            return jnp.einsum("sij,sjc->ic", blocks.astype(jnp.float32), picked.astype(jnp.float32))

        product = lax.map(one_row, (hamiltonian_blocks, block_columns)).reshape(total, -1)
        upcoming = 2.0 * product - previous
        results.append(jnp.sum(weights * upcoming, axis=0))
        previous, current = current, upcoming
    return previous, current, jnp.stack(results)
```

```python
import functools

import jax
import jax.numpy as jnp
from jax import lax
from jax.experimental import pallas as pl
from jax.experimental.pallas import tpu as pltpu
from jax.sharding import PartitionSpec as P

BAND = 5
TERMS = 3
LANES = 128
CHUNK = 256
GROUP = 2


def kernel(
    n, col_ref, ow_ref, h_hbm, probe_hbm, prev_hbm, cur_hbm,
    last_prev, last_cur, mom_ref,
    hv, hb, ext, tb, wts, pv, mom,
    in_sem, out_sem, send_sem, recv_sem, msend, mrecv,
):
    me = lax.axis_index("slab")
    rows, slots, w, _ = hv.shape
    chunks, height, cc = wts.shape
    total = n * rows
    rim = BAND * w
    gw = GROUP * w
    pairs = rows // GROUP
    edge = -(-BAND // GROUP)
    depth = gw + 2 * rim
    first = me * rows
    low, high = lax.rem(me + n - 1, n), lax.rem(me + 1, n)

    def columns(c):
        return pl.ds(c * cc, cc)

    pieces = ((0, rim), (height - rim, rim), (rim, height - 2 * rim))
    cur_in = {}
    for c in range(chunks):
        for k, (start, size) in enumerate(pieces):
            cur_in[c, k] = pltpu.make_async_copy(
                cur_hbm.at[pl.ds(start, size), columns(c)],
                tb.at[1, c, pl.ds(start, size)],
                in_sem.at[3 * c + k],
            )
    base = 3 * chunks
    h_in = pltpu.make_async_copy(h_hbm, hv, in_sem.at[base])
    probe_in = pltpu.make_async_copy(probe_hbm, pv, in_sem.at[base + 1])
    prev_in = [
        pltpu.make_async_copy(prev_hbm.at[:, columns(c)], tb.at[0, c], in_sem.at[base + 2 + c])
        for c in range(chunks)
    ]
    for c in range(chunks):
        cur_in[c, 0].start()
        cur_in[c, 1].start()

    barrier = pltpu.get_barrier_semaphore()
    for k in range(1, n):
        pl.semaphore_signal(
            barrier, inc=1, device_id={"slab": lax.rem(me + k, n)},
            device_id_type=pl.DeviceIdType.MESH,
        )

    def halo(t, c):
        down = pltpu.make_async_remote_copy(
            src_ref=ext.at[t, c, pl.ds(rim, rim)],
            dst_ref=ext.at[t, c, pl.ds(rim + height, rim)],
            send_sem=send_sem.at[t, c, 0], recv_sem=recv_sem.at[t, c, 0],
            device_id={"slab": low}, device_id_type=pl.DeviceIdType.MESH,
        )
        up = pltpu.make_async_remote_copy(
            src_ref=ext.at[t, c, pl.ds(height, rim)],
            dst_ref=ext.at[t, c, pl.ds(0, rim)],
            send_sem=send_sem.at[t, c, 1], recv_sem=recv_sem.at[t, c, 1],
            device_id={"slab": high}, device_id_type=pl.DeviceIdType.MESH,
        )
        return down, up

    def cast(c, k):
        start, size = pieces[k]
        steps = size // w

        def body(i, carry):
            at = pl.multiple_of(start + i * w, w)
            ext[0, c, pl.ds(pl.multiple_of(rim + at, w), w)] = tb[1, c, pl.ds(at, w)].astype(jnp.bfloat16)
            return carry

        lax.fori_loop(0, steps, body, 0)

    halos = {(t, c): halo(t, c) for t in range(TERMS) for c in range(chunks)}
    for c in range(chunks):
        cur_in[c, 0].wait()
        cur_in[c, 1].wait()
        if c == 0:
            for k in range(chunks):
                cur_in[k, 2].start()
            h_in.start()
            probe_in.start()
            for copy in prev_in:
                copy.start()
        cast(c, 0)
        cast(c, 1)
        if c == 0:
            pl.semaphore_wait(barrier, n - 1)
        for copy in halos[0, c]:
            copy.start()
    for c in range(chunks):
        cur_in[c, 2].wait()
        cast(c, 2)

    h_in.wait()
    zero = jnp.zeros((w, w), jnp.bfloat16)

    def build(p, carry):
        for half in range(GROUP):
            r = p * GROUP + half
            places = []
            for s in range(slots):
                x = col_ref[r, s] - (first + r) + BAND
                x = jnp.where(x < 0, x + total, x)
                places.append(jnp.where(x >= total, x - total, x))
            for d in range(GROUP + 2 * BAND):
                place = d - half
                if place < 0 or place > 2 * BAND:
                    block = zero
                else:
                    slot = jnp.int32(0)
                    hit = jnp.int32(0)
                    for s in range(slots):
                        same = places[s] == place
                        slot = jnp.where(same, s, slot)
                        hit = jnp.where(same, 1, hit)
                    block = jnp.where(hit == 1, hv[r, slot], zero)
                hb[p, half * w:(half + 1) * w, d * w:(d + 1) * w] = block
        return carry

    lax.fori_loop(0, pairs, build, 0)

    probe_in.wait()
    eye = lax.broadcasted_iota(jnp.int32, (w, w), 0) == lax.broadcasted_iota(jnp.int32, (w, w), 1)

    def weigh(r, carry):
        row = jnp.broadcast_to(ow_ref[pl.ds(r, 1), :], (w, w))
        column = jnp.sum(jnp.where(eye, row, 0.0), axis=1, keepdims=True) / (total * w)
        at = pl.multiple_of(r * w, w)
        for c in range(chunks):
            wts[c, pl.ds(at, w)] = column * pv[pl.ds(at, w), c * cc:(c + 1) * cc].astype(jnp.float32)
        return carry

    lax.fori_loop(0, rows, weigh, 0)
    for copy in prev_in:
        copy.wait()

    def tile(t, c, p, acc):
        at = pl.multiple_of(p * gw, gw)
        product = jnp.dot(hb[p], ext[t, c, pl.ds(at, depth)], preferred_element_type=jnp.float32)
        upcoming = 2.0 * product - tb[t % 2, c, pl.ds(at, gw)]
        tb[t % 2, c, pl.ds(at, gw)] = upcoming
        if t + 1 < TERMS:
            ext[t + 1, c, pl.ds(pl.multiple_of(rim + at, w), gw)] = upcoming.astype(jnp.bfloat16)
        y = wts[c, pl.ds(at, gw)] * upcoming
        return acc + jnp.sum(y.reshape(gw // 8, 8, cc), axis=0)

    def sums(t):
        return [
            pltpu.make_async_remote_copy(
                src_ref=mom.at[t, me], dst_ref=mom.at[t, me],
                send_sem=msend.at[t, k], recv_sem=mrecv.at[t, k],
                device_id={"slab": lax.rem(me + k, n)}, device_id_type=pl.DeviceIdType.MESH,
            )
            for k in range(1, n)
        ]

    outs = []
    sent = []
    mid_at, mid_size = edge * gw, height - 2 * edge * gw
    for t in range(TERMS):
        for c in range(chunks):
            acc = jnp.zeros((8, cc), jnp.float32)
            acc = lax.fori_loop(edge, pairs - edge, lambda p, a: tile(t, c, p, a), acc)
            for copy in halos[t, c]:
                copy.wait()
            if t == TERMS - 1:
                copy = pltpu.make_async_copy(
                    tb.at[t % 2, c, pl.ds(mid_at, mid_size)],
                    last_cur.at[pl.ds(mid_at, mid_size), columns(c)], out_sem.at[c, 0])
                copy.start()
                outs.append(copy)
            acc = lax.fori_loop(
                0, 2 * edge,
                lambda i, a: tile(t, c, jnp.where(i < edge, i, i + (pairs - 2 * edge)), a), acc)
            if t + 1 < TERMS:
                for copy in halos[t + 1, c]:
                    copy.start()
            total_row = jnp.sum(acc, axis=0, keepdims=True)
            for k in range(cc // LANES):
                mom[t, me, pl.ds(c * (cc // LANES) + k, 1), :] = total_row[:, k * LANES:(k + 1) * LANES]
            if t == TERMS - 2:
                copy = pltpu.make_async_copy(tb.at[t % 2, c], last_prev.at[:, columns(c)], out_sem.at[c, 3])
                copy.start()
                outs.append(copy)
            if t == TERMS - 1:
                for k, start in ((1, 0), (2, height - mid_at)):
                    copy = pltpu.make_async_copy(
                        tb.at[t % 2, c, pl.ds(start, mid_at)],
                        last_cur.at[pl.ds(start, mid_at), columns(c)], out_sem.at[c, k])
                    copy.start()
                    outs.append(copy)
        copies = sums(t)
        for copy in copies:
            copy.start()
        sent.append(copies)

    for t in range(TERMS):
        for copy in sent[t]:
            copy.wait()
        whole = mom[t, 0]
        for i in range(1, n):
            whole = whole + mom[t, i]
        for k in range(whole.shape[0]):
            mom_ref[t:t + 1, k * LANES:(k + 1) * LANES] = whole[k:k + 1, :]
    for copy in outs:
        copy.wait()


def local(hamiltonian_blocks, block_columns, probe, previous, current, orbital_weight):
    n = lax.axis_size("slab")
    rows, slots, w, _ = hamiltonian_blocks.shape
    height, cols = current.shape
    cc = min(CHUNK, cols)
    chunks = cols // cc
    vmem = pl.BlockSpec(memory_space=pltpu.VMEM)
    hbm = pl.BlockSpec(memory_space=pl.ANY)
    bf16, f32 = jnp.bfloat16, jnp.float32
    return pl.pallas_call(
        functools.partial(kernel, n),
        out_shape=(
            jax.ShapeDtypeStruct((height, cols), f32),
            jax.ShapeDtypeStruct((height, cols), f32),
            jax.ShapeDtypeStruct((TERMS, cols), f32),
        ),
        in_specs=[pl.BlockSpec(memory_space=pltpu.SMEM), vmem, hbm, hbm, hbm, hbm],
        out_specs=(hbm, hbm, vmem),
        scratch_shapes=[
            pltpu.VMEM((rows, slots, w, w), bf16),
            pltpu.VMEM((rows // GROUP, GROUP * w, (GROUP + 2 * BAND) * w), bf16),
            pltpu.VMEM((TERMS, chunks, height + 2 * BAND * w, cc), bf16),
            pltpu.VMEM((2, chunks, height, cc), f32),
            pltpu.VMEM((chunks, height, cc), f32),
            pltpu.VMEM((height, cols), bf16),
            pltpu.VMEM((TERMS, n, cols // LANES, LANES), f32),
            pltpu.SemaphoreType.DMA((4 * chunks + 2,)),
            pltpu.SemaphoreType.DMA((chunks, 4)),
            pltpu.SemaphoreType.DMA((TERMS, chunks, 2)),
            pltpu.SemaphoreType.DMA((TERMS, chunks, 2)),
            pltpu.SemaphoreType.DMA((TERMS, n)),
            pltpu.SemaphoreType.DMA((TERMS, n)),
        ],
        compiler_params=pltpu.CompilerParams(
            collective_id=0, has_side_effects=True, vmem_limit_bytes=48 * 1024 * 1024,
        ),
    )(block_columns, orbital_weight.reshape(rows, w), hamiltonian_blocks, probe, previous, current)


def solution(mesh):
    return jax.shard_map(
        local,
        mesh=mesh,
        in_specs=(
            P("slab", None, None, None),
            P("slab", None),
            P("slab", "col"),
            P("slab", "col"),
            P("slab", "col"),
            P("slab"),
        ),
        out_specs=(P("slab", "col"), P("slab", "col"), P(None, "col")),
        check_vma=False,
    )
```

```python
import functools

import jax
import jax.numpy as jnp
from jax import lax
from jax.experimental import pallas as pl
from jax.experimental.pallas import tpu as pltpu
from jax.sharding import PartitionSpec as P

BAND = 5
TERMS = 3
LANES = 128
CHUNK = 256
GROUP = 2


def kernel(
    n, col_hbm, ow_hbm, h_hbm, probe_hbm, prev_hbm, cur_hbm,
    tb, mom,
    col_ref, ow_ref, hv, hb, ext, wts, pv,
    in_sem, send_sem, recv_sem, msend, mrecv,
):
    me = lax.axis_index("slab")
    rows, slots, w, _ = hv.shape
    chunks, height, cc = wts.shape
    total = n * rows
    rim = BAND * w
    gw = GROUP * w
    pairs = rows // GROUP
    edge = -(-BAND // GROUP)
    depth = gw + 2 * rim
    first = me * rows
    far = lax.rem(me, 2)
    near = 1 - far

    def columns(c):
        return pl.ds(c * cc, cc)

    def rim_in(c, side):
        start = pl.multiple_of(side * (height - rim), w)
        return pltpu.make_async_copy(
            cur_hbm.at[pl.ds(start, rim), columns(c)],
            tb.at[1, c, pl.ds(start, rim)],
            in_sem.at[3 * c + side],
        )

    inner = height - 2 * rim
    inner_in = [
        pltpu.make_async_copy(
            cur_hbm.at[pl.ds(rim, inner), columns(c)], tb.at[1, c, pl.ds(rim, inner)],
            in_sem.at[3 * c + 2])
        for c in range(chunks)
    ]
    base = 3 * chunks
    h_in = pltpu.make_async_copy(h_hbm, hv, in_sem.at[base])
    probe_in = pltpu.make_async_copy(probe_hbm, pv, in_sem.at[base + 1])
    col_in = pltpu.make_async_copy(col_hbm, col_ref, in_sem.at[base + 2])
    ow_in = pltpu.make_async_copy(ow_hbm, ow_ref, in_sem.at[base + 3])
    prev_in = [
        pltpu.make_async_copy(prev_hbm.at[:, columns(c)], tb.at[0, c], in_sem.at[base + 4 + c])
        for c in range(chunks)
    ]
    for c in range(chunks):
        rim_in(c, far).start()
        rim_in(c, near).start()

    barrier = pltpu.get_barrier_semaphore()
    for k in range(1, n):
        pl.semaphore_signal(
            barrier, inc=1, device_id={"slab": lax.rem(me + k, n)},
            device_id_type=pl.DeviceIdType.MESH,
        )

    def halo(t, c, side):
        source = pl.multiple_of(rim + side * (height - rim), w)
        target = pl.multiple_of((1 - side) * (rim + height), w)
        return pltpu.make_async_remote_copy(
            src_ref=ext.at[t, c, pl.ds(source, rim)],
            dst_ref=ext.at[t, c, pl.ds(target, rim)],
            send_sem=send_sem.at[t, c, side], recv_sem=recv_sem.at[t, c, 1 - side],
            device_id={"slab": lax.rem(me + n - 1 + 2 * side, n)},
            device_id_type=pl.DeviceIdType.MESH,
        )

    def cast(c, start, steps):
        def body(i, carry):
            at = pl.multiple_of(start + i * w, w)
            ext[0, c, pl.ds(pl.multiple_of(rim + at, w), w)] = tb[1, c, pl.ds(at, w)].astype(jnp.bfloat16)
            return carry

        lax.fori_loop(0, steps, body, 0)

    for c in range(chunks):
        for side in (far, near):
            rim_in(c, side).wait()
            cast(c, side * (height - rim), BAND)
            if c == 0 and side is far:
                for copy in inner_in:
                    copy.start()
                col_in.start()
                h_in.start()
                ow_in.start()
                probe_in.start()
                for copy in prev_in:
                    copy.start()
                pl.semaphore_wait(barrier, n - 1)
            halo(0, c, side).start()
    for c in range(chunks):
        inner_in[c].wait()
        cast(c, rim, inner // w)

    col_in.wait()
    h_in.wait()
    zero = jnp.zeros((w, w), jnp.bfloat16)

    def build(p, carry):
        for half in range(GROUP):
            r = p * GROUP + half
            places = []
            for s in range(slots):
                x = col_ref[r, s] - (first + r) + BAND
                x = jnp.where(x < 0, x + total, x)
                places.append(jnp.where(x >= total, x - total, x))
            for d in range(GROUP + 2 * BAND):
                place = d - half
                if place < 0 or place > 2 * BAND:
                    block = zero
                else:
                    slot = jnp.int32(0)
                    hit = jnp.int32(0)
                    for s in range(slots):
                        same = places[s] == place
                        slot = jnp.where(same, s, slot)
                        hit = jnp.where(same, 1, hit)
                    block = jnp.where(hit == 1, hv[r, slot], zero)
                hb[p, half * w:(half + 1) * w, d * w:(d + 1) * w] = block
        return carry

    lax.fori_loop(0, pairs, build, 0)

    probe_in.wait()
    ow_in.wait()
    eye = lax.broadcasted_iota(jnp.int32, (w, w), 0) == lax.broadcasted_iota(jnp.int32, (w, w), 1)

    def weigh(r, carry):
        row = jnp.broadcast_to(ow_ref[pl.ds(r, 1), :], (w, w))
        column = jnp.sum(jnp.where(eye, row, 0.0), axis=1, keepdims=True) / (total * w)
        at = pl.multiple_of(r * w, w)
        for c in range(chunks):
            wts[c, pl.ds(at, w)] = column * pv[pl.ds(at, w), c * cc:(c + 1) * cc].astype(jnp.float32)
        return carry

    lax.fori_loop(0, rows, weigh, 0)
    for copy in prev_in:
        copy.wait()

    def tile(t, c, p, acc):
        at = pl.multiple_of(p * gw, gw)
        product = jnp.dot(hb[p], ext[t, c, pl.ds(at, depth)], preferred_element_type=jnp.float32)
        upcoming = 2.0 * product - tb[t % 2, c, pl.ds(at, gw)]
        tb[t % 2, c, pl.ds(at, gw)] = upcoming
        if t + 1 < TERMS:
            ext[t + 1, c, pl.ds(pl.multiple_of(rim + at, w), gw)] = upcoming.astype(jnp.bfloat16)
        y = wts[c, pl.ds(at, gw)] * upcoming
        return acc + jnp.sum(y.reshape(gw // 8, 8, cc), axis=0)

    def sums(t):
        return [
            pltpu.make_async_remote_copy(
                src_ref=mom.at[t, me], dst_ref=mom.at[t, me],
                send_sem=msend.at[t, k], recv_sem=mrecv.at[t, k],
                device_id={"slab": lax.rem(me + k, n)}, device_id_type=pl.DeviceIdType.MESH,
            )
            for k in range(1, n)
        ]

    sent = []
    for t in range(TERMS):
        for c in range(chunks):
            acc = jnp.zeros((8, cc), jnp.float32)
            acc = lax.fori_loop(edge, pairs - edge, lambda p, a: tile(t, c, p, a), acc)
            for side in (near, far):
                halo(t, c, 1 - side).wait_recv()
                acc = lax.fori_loop(
                    0, edge, lambda i, a: tile(t, c, i + side * (pairs - edge), a), acc)
                if t + 1 < TERMS:
                    halo(t + 1, c, side).start()
            total_row = jnp.sum(acc, axis=0, keepdims=True)
            for k in range(cc // LANES):
                mom[t, me, pl.ds(c * (cc // LANES) + k, 1), :] = total_row[:, k * LANES:(k + 1) * LANES]
        copies = sums(t)
        for copy in copies:
            copy.start()
        sent.append(copies)

    for t in range(TERMS):
        for c in range(chunks):
            for side in (near, far):
                halo(t, c, side).wait_send()
    for copies in sent:
        for copy in copies:
            copy.wait()


def finish(tb, mom, last_prev, last_cur, mom_hbm, row_sums, sem):
    terms, n, lanes_of, _ = mom.shape
    _, chunks, _, cc = tb.shape
    copies = []
    for c in range(chunks):
        for k, out in enumerate((last_cur, last_prev)):
            source = (terms - 1 + k) % 2
            copies.append(pltpu.make_async_copy(
                tb.at[source, c], out.at[:, pl.ds(c * cc, cc)], sem.at[2 * c + k]))
    for copy in copies:
        copy.start()
    for t in range(terms):
        whole = mom[t, 0]
        for i in range(1, n):
            whole = whole + mom[t, i]
        for k in range(lanes_of):
            row_sums[t:t + 1, k * LANES:(k + 1) * LANES] = whole[k:k + 1, :]
    copies.append(pltpu.make_async_copy(row_sums, mom_hbm, sem.at[2 * chunks]))
    copies[-1].start()
    for copy in copies:
        copy.wait()


def local(hamiltonian_blocks, block_columns, probe, previous, current, orbital_weight):
    n = lax.axis_size("slab")
    rows, slots, w, _ = hamiltonian_blocks.shape
    height, cols = current.shape
    cc = min(CHUNK, cols)
    chunks = cols // cc
    vmem = pl.BlockSpec(memory_space=pltpu.VMEM)
    hbm = pl.BlockSpec(memory_space=pltpu.HBM)
    bf16, f32 = jnp.bfloat16, jnp.float32
    tb, mom = pl.pallas_call(
        functools.partial(kernel, n),
        out_shape=(
            pltpu.VMEM((2, chunks, height, cc), f32),
            pltpu.VMEM((TERMS, n, cols // LANES, LANES), f32),
        ),
        in_specs=[hbm] * 6,
        out_specs=(vmem, vmem),
        scratch_shapes=[
            pltpu.SMEM((rows, slots), jnp.int32),
            pltpu.VMEM((rows, w), f32),
            pltpu.VMEM((rows, slots, w, w), bf16),
            pltpu.VMEM((rows // GROUP, GROUP * w, (GROUP + 2 * BAND) * w), bf16),
            pltpu.VMEM((TERMS, chunks, height + 2 * BAND * w, cc), bf16),
            pltpu.VMEM((chunks, height, cc), f32),
            pltpu.VMEM((height, cols), bf16),
            pltpu.SemaphoreType.DMA((4 * chunks + 4,)),
            pltpu.SemaphoreType.DMA((TERMS, chunks, 2)),
            pltpu.SemaphoreType.DMA((TERMS, chunks, 2)),
            pltpu.SemaphoreType.DMA((TERMS, n)),
            pltpu.SemaphoreType.DMA((TERMS, n)),
        ],
        compiler_params=pltpu.CompilerParams(
            collective_id=0, has_side_effects=True, vmem_limit_bytes=44 * 1024 * 1024,
        ),
    )(block_columns, orbital_weight.reshape(rows, w), hamiltonian_blocks, probe, previous, current)
    return pl.pallas_call(
        finish,
        out_shape=(
            jax.ShapeDtypeStruct((height, cols), f32),
            jax.ShapeDtypeStruct((height, cols), f32),
            jax.ShapeDtypeStruct((TERMS, cols), f32),
        ),
        in_specs=[vmem, vmem],
        out_specs=(hbm, hbm, hbm),
        scratch_shapes=[
            pltpu.VMEM((TERMS, cols), f32),
            pltpu.SemaphoreType.DMA((2 * chunks + 1,)),
        ],
        compiler_params=pltpu.CompilerParams(vmem_limit_bytes=16 * 1024 * 1024),
    )(tb, mom)


def solution(mesh):
    return jax.shard_map(
        local,
        mesh=mesh,
        in_specs=(
            P("slab", None, None, None),
            P("slab", None),
            P("slab", "col"),
            P("slab", "col"),
            P("slab", "col"),
            P("slab"),
        ),
        out_specs=(P("slab", "col"), P("slab", "col"), P(None, "col")),
        check_vma=False,
    )
```

```python
import functools

import jax
import jax.numpy as jnp
from jax import lax
from jax.experimental import pallas as pl
from jax.experimental.pallas import tpu as pltpu
from jax.sharding import PartitionSpec as P

BAND = 5
TERMS = 3
LANES = 128
CHUNK = 256
GROUP = 2


def kernel(
    n, col_hbm, ow_hbm, h_hbm, probe_hbm, prev_hbm, cur_hbm,
    tb, mom,
    col_ref, ow_ref, hv, hb, ext, wts, pv,
    in_sem, send_sem, recv_sem, msend, mrecv,
):
    me = lax.axis_index("slab")
    rows, slots, w, _ = hv.shape
    chunks, height, cc = wts.shape
    total = n * rows
    rim = BAND * w
    gw = GROUP * w
    pairs = rows // GROUP
    edge = -(-BAND // GROUP)
    depth = gw + 2 * rim
    first = me * rows
    far = lax.rem(me, 2)
    near = 1 - far

    def columns(c):
        return pl.ds(c * cc, cc)

    def rim_in(c, side):
        start = pl.multiple_of(side * (height - rim), w)
        return pltpu.make_async_copy(
            cur_hbm.at[pl.ds(start, rim), columns(c)],
            tb.at[1, c, pl.ds(start, rim)],
            in_sem.at[3 * c + side],
        )

    inner = height - 2 * rim
    inner_in = [
        pltpu.make_async_copy(
            cur_hbm.at[pl.ds(rim, inner), columns(c)], tb.at[1, c, pl.ds(rim, inner)],
            in_sem.at[3 * c + 2])
        for c in range(chunks)
    ]
    base = 3 * chunks
    h_in = pltpu.make_async_copy(h_hbm, hv, in_sem.at[base])
    probe_in = pltpu.make_async_copy(probe_hbm, pv, in_sem.at[base + 1])
    col_in = pltpu.make_async_copy(col_hbm, col_ref, in_sem.at[base + 2])
    ow_in = pltpu.make_async_copy(ow_hbm, ow_ref, in_sem.at[base + 3])
    prev_in = [
        pltpu.make_async_copy(prev_hbm.at[:, columns(c)], tb.at[0, c], in_sem.at[base + 4 + c])
        for c in range(chunks)
    ]
    for c in range(chunks):
        rim_in(c, far).start()
        rim_in(c, near).start()

    barrier = pltpu.get_barrier_semaphore()
    for k in range(1, n):
        pl.semaphore_signal(
            barrier, inc=1, device_id={"slab": lax.rem(me + k, n)},
            device_id_type=pl.DeviceIdType.MESH,
        )

    inside = BAND - GROUP

    def halo(t, c, side, part):
        size = (BAND - inside if part else inside) * w
        offset = (1 - side) * inside * w if part else side * (BAND - inside) * w
        source = pl.multiple_of(rim + side * (height - rim) + offset, w)
        target = pl.multiple_of((1 - side) * (rim + height) + offset, w)
        return pltpu.make_async_remote_copy(
            src_ref=ext.at[t, c, pl.ds(source, size)],
            dst_ref=ext.at[t, c, pl.ds(target, size)],
            send_sem=send_sem.at[t, c, side, part], recv_sem=recv_sem.at[t, c, 1 - side, part],
            device_id={"slab": lax.rem(me + n - 1 + 2 * side, n)},
            device_id_type=pl.DeviceIdType.MESH,
        )

    def cast(c, start, steps):
        def body(i, carry):
            at = pl.multiple_of(start + i * w, w)
            ext[0, c, pl.ds(pl.multiple_of(rim + at, w), w)] = tb[1, c, pl.ds(at, w)].astype(jnp.bfloat16)
            return carry

        lax.fori_loop(0, steps, body, 0)

    for c in range(chunks):
        for side in (far, near):
            rim_in(c, side).wait()
            cast(c, side * (height - rim), BAND)
            if c == 0 and side is far:
                for copy in inner_in:
                    copy.start()
                col_in.start()
                h_in.start()
                ow_in.start()
                probe_in.start()
                for copy in prev_in:
                    copy.start()
                pl.semaphore_wait(barrier, n - 1)
            for part in range(2):
                halo(0, c, side, part).start()
    for c in range(chunks):
        inner_in[c].wait()
        cast(c, rim, inner // w)

    col_in.wait()
    h_in.wait()
    zero = jnp.zeros((w, w), jnp.bfloat16)

    def build(p, carry):
        for half in range(GROUP):
            r = p * GROUP + half
            places = []
            for s in range(slots):
                x = col_ref[r, s] - (first + r) + BAND
                x = jnp.where(x < 0, x + total, x)
                places.append(jnp.where(x >= total, x - total, x))
            for d in range(GROUP + 2 * BAND):
                place = d - half
                if place < 0 or place > 2 * BAND:
                    block = zero
                else:
                    slot = jnp.int32(0)
                    hit = jnp.int32(0)
                    for s in range(slots):
                        same = places[s] == place
                        slot = jnp.where(same, s, slot)
                        hit = jnp.where(same, 1, hit)
                    block = jnp.where(hit == 1, hv[r, slot], zero)
                hb[p, half * w:(half + 1) * w, d * w:(d + 1) * w] = block
        return carry

    lax.fori_loop(0, pairs, build, 0)

    probe_in.wait()
    ow_in.wait()
    eye = lax.broadcasted_iota(jnp.int32, (w, w), 0) == lax.broadcasted_iota(jnp.int32, (w, w), 1)

    def weigh(r, carry):
        row = jnp.broadcast_to(ow_ref[pl.ds(r, 1), :], (w, w))
        column = jnp.sum(jnp.where(eye, row, 0.0), axis=1, keepdims=True) / (total * w)
        at = pl.multiple_of(r * w, w)
        for c in range(chunks):
            wts[c, pl.ds(at, w)] = column * pv[pl.ds(at, w), c * cc:(c + 1) * cc].astype(jnp.float32)
        return carry

    lax.fori_loop(0, rows, weigh, 0)
    for copy in prev_in:
        copy.wait()

    def tile(t, c, p, acc):
        at = pl.multiple_of(p * gw, gw)
        product = jnp.dot(hb[p], ext[t, c, pl.ds(at, depth)], preferred_element_type=jnp.float32)
        upcoming = 2.0 * product - tb[t % 2, c, pl.ds(at, gw)]
        tb[t % 2, c, pl.ds(at, gw)] = upcoming
        if t + 1 < TERMS:
            ext[t + 1, c, pl.ds(pl.multiple_of(rim + at, w), gw)] = upcoming.astype(jnp.bfloat16)
        y = wts[c, pl.ds(at, gw)] * upcoming
        return acc + jnp.sum(y.reshape(gw // 8, 8, cc), axis=0)

    def sums(t):
        return [
            pltpu.make_async_remote_copy(
                src_ref=mom.at[t, me], dst_ref=mom.at[t, me],
                send_sem=msend.at[t, k], recv_sem=mrecv.at[t, k],
                device_id={"slab": lax.rem(me + k, n)}, device_id_type=pl.DeviceIdType.MESH,
            )
            for k in range(1, n)
        ]

    sent = []
    for t in range(TERMS):
        for c in range(chunks):
            acc = jnp.zeros((8, cc), jnp.float32)
            acc = lax.fori_loop(edge, pairs - edge, lambda p, a: tile(t, c, p, a), acc)
            for side in (near, far):
                def rim_tile(i, a):
                    return tile(t, c, (1 - side) * (edge - 1 - i) + side * (pairs - edge + i), a)

                halo(t, c, 1 - side, 0).wait_recv()
                acc = lax.fori_loop(0, edge - 1, rim_tile, acc)
                halo(t, c, 1 - side, 1).wait_recv()
                acc = rim_tile(edge - 1, acc)
                if t + 1 < TERMS:
                    for part in range(2):
                        halo(t + 1, c, side, part).start()
            total_row = jnp.sum(acc, axis=0, keepdims=True)
            for k in range(cc // LANES):
                mom[t, me, pl.ds(c * (cc // LANES) + k, 1), :] = total_row[:, k * LANES:(k + 1) * LANES]
        copies = sums(t)
        for copy in copies:
            copy.start()
        sent.append(copies)

    for t in range(TERMS):
        for c in range(chunks):
            for side in (near, far):
                for part in range(2):
                    halo(t, c, side, part).wait_send()
    for copies in sent:
        for copy in copies:
            copy.wait()


def finish(tb, mom, last_prev, last_cur, mom_hbm, row_sums, sem):
    terms, n, lanes_of, _ = mom.shape
    _, chunks, _, cc = tb.shape
    copies = []
    for c in range(chunks):
        for k, out in enumerate((last_cur, last_prev)):
            source = (terms - 1 + k) % 2
            copies.append(pltpu.make_async_copy(
                tb.at[source, c], out.at[:, pl.ds(c * cc, cc)], sem.at[2 * c + k]))
    for copy in copies:
        copy.start()
    for t in range(terms):
        whole = mom[t, 0]
        for i in range(1, n):
            whole = whole + mom[t, i]
        for k in range(lanes_of):
            row_sums[t:t + 1, k * LANES:(k + 1) * LANES] = whole[k:k + 1, :]
    copies.append(pltpu.make_async_copy(row_sums, mom_hbm, sem.at[2 * chunks]))
    copies[-1].start()
    for copy in copies:
        copy.wait()


def local(hamiltonian_blocks, block_columns, probe, previous, current, orbital_weight):
    n = lax.axis_size("slab")
    rows, slots, w, _ = hamiltonian_blocks.shape
    height, cols = current.shape
    cc = min(CHUNK, cols)
    chunks = cols // cc
    vmem = pl.BlockSpec(memory_space=pltpu.VMEM)
    hbm = pl.BlockSpec(memory_space=pltpu.HBM)
    bf16, f32 = jnp.bfloat16, jnp.float32
    grant = 67043328 - 4 * (2 * height * cols + TERMS * n * cols) - (64 << 10)
    tb, mom = pl.pallas_call(
        functools.partial(kernel, n),
        out_shape=(
            pltpu.VMEM((2, chunks, height, cc), f32),
            pltpu.VMEM((TERMS, n, cols // LANES, LANES), f32),
        ),
        in_specs=[hbm] * 6,
        out_specs=(vmem, vmem),
        scratch_shapes=[
            pltpu.SMEM((rows, slots), jnp.int32),
            pltpu.VMEM((rows, w), f32),
            pltpu.VMEM((rows, slots, w, w), bf16),
            pltpu.VMEM((rows // GROUP, GROUP * w, (GROUP + 2 * BAND) * w), bf16),
            pltpu.VMEM((TERMS, chunks, height + 2 * BAND * w, cc), bf16),
            pltpu.VMEM((chunks, height, cc), f32),
            pltpu.VMEM((height, cols), bf16),
            pltpu.SemaphoreType.DMA((4 * chunks + 4,)),
            pltpu.SemaphoreType.DMA((TERMS, chunks, 2, 2)),
            pltpu.SemaphoreType.DMA((TERMS, chunks, 2, 2)),
            pltpu.SemaphoreType.DMA((TERMS, n)),
            pltpu.SemaphoreType.DMA((TERMS, n)),
        ],
        compiler_params=pltpu.CompilerParams(
            collective_id=0, has_side_effects=True, vmem_limit_bytes=grant,
        ),
    )(block_columns, orbital_weight.reshape(rows, w), hamiltonian_blocks, probe, previous, current)
    return pl.pallas_call(
        finish,
        out_shape=(
            jax.ShapeDtypeStruct((height, cols), f32),
            jax.ShapeDtypeStruct((height, cols), f32),
            jax.ShapeDtypeStruct((TERMS, cols), f32),
        ),
        in_specs=[vmem, vmem],
        out_specs=(hbm, hbm, hbm),
        scratch_shapes=[
            pltpu.VMEM((TERMS, cols), f32),
            pltpu.SemaphoreType.DMA((2 * chunks + 1,)),
        ],
        compiler_params=pltpu.CompilerParams(vmem_limit_bytes=16 * 1024 * 1024),
    )(tb, mom)


def solution(mesh):
    return jax.shard_map(
        local,
        mesh=mesh,
        in_specs=(
            P("slab", None, None, None),
            P("slab", None),
            P("slab", "col"),
            P("slab", "col"),
            P("slab", "col"),
            P("slab"),
        ),
        out_specs=(P("slab", "col"), P("slab", "col"), P(None, "col")),
        check_vma=False,
    )
```
